128 devices in a mesh: ctx: 16 (over y, x), tp: 8 (over z, core).
Axes of the slice: x: 4, y: 4, z: 4, core: 2. Of those that a mesh axis runs over, the one named last changes fastest.
Arguments:
- hidden: bfloat16 [8, 8192], P(None, 'ctx'), may hold values from -4.8 to 4.8, as said below
- norm_gains: bfloat16 [4, 8192], P(None, 'ctx'), may hold values from 0.5 to 1.5
- w_query: bfloat16 [4, 8192, 8192], P(None, 'ctx', 'tp'), may hold values from -0.0625 to 0.0625
- w_key: bfloat16 [4, 8192, 1024], P(None, 'ctx', 'tp'), may hold values from -0.125 to 0.125
- w_value: bfloat16 [4, 8192, 1024], P(None, 'ctx', 'tp'), may hold values from -0.125 to 0.125
- w_out: bfloat16 [4, 8192, 8192], P(None, 'tp', 'ctx'), may hold values from -0.0625 to 0.0625
- key_cache: bfloat16 [4, 8, 8, 2048, 128], P(None, None, 'tp', 'ctx'), may hold values from -9 to 9
- value_cache: bfloat16 [4, 8, 8, 2048, 128], P(None, None, 'tp', 'ctx'), may hold values from -6 to 6
- lengths: int32 [8], replicated, may hold values from 1 to 2048, 8200 in all
Outputs:
- updated: float32 [8, 8192], P(None, 'ctx')
The draws below stay inside these ranges and needn't reach their ends.
Inputs may be any that keep to these rules, and one draw needn't show every extreme that they name: Each sequence has lengths[b] valid cache positions 0 .. lengths[b] - 1, between 1 and 2048; the longest sequence has exactly 2048; the new token sits at position lengths[b]. `hidden`: activations of order 0.2; in each block of 512 consecutive features one sequence, chosen at random, has entries four times larger.
All inputs are finite; a program needn't handle non-finite values.
Results may differ from the reference program's by a relative error of at most 0.02.
Values sent between devices are 32-bit elements.
No kernel may reach another device: no remote copies, remote signals or barrier semaphores. Data moves between devices by JAX's collectives and lax.ppermute only.
A program may use at most 64 MiB of HBM per device.

```python
import math
import jax
import jax.numpy as jnp
import numpy as np
from jax import lax

D = 8192
HQ = 64
KVH = 8
HD = 128
LAYERS = 4
BATCH = 8
CAP = 2048
D_DEV = 512


def draw_hidden(key, part):
    base_key, owner_key = jax.random.split(jax.random.fold_in(key, 7))
    block_count = D // D_DEV
    owners = jax.random.randint(owner_key, (block_count,), 0, BATCH)
    column_owner = owners[jnp.arange(D) // D_DEV]
    factor = jnp.where(column_owner[None, :] == jnp.arange(BATCH)[:, None], 4.0, 1.0)
    base_draw = jnp.clip(jax.random.normal(base_key, (BATCH, D), jnp.float32), -6.0, 6.0)
    return (0.2 * factor * base_draw).astype(jnp.bfloat16)


def block_scale(rng, extent, pieces, smallest, high):
    gain = 1.0
    for axis_at, parts in pieces:
        draws = jax.random.uniform(jax.random.fold_in(jax.random.fold_in(rng, 6), axis_at), (parts,), jnp.float32, smallest / len(pieces), high / len(pieces))
        gain = gain * jnp.repeat(jnp.exp(draws), extent[axis_at] // parts).reshape((-1,) + (1,) * (len(extent) - 1 - axis_at))
    return gain


def profile(count, total, reach, slope):
    portions = [(1 << 20) // math.isqrt(grade ** slope) + 1 for grade in range(2, count + 1)]
    surplus, given = total - reach - (count - 1), [1] * (count - 1)
    while surplus > 0:
        movable = [i for i in range(count - 1) if given[i] < reach]
        mass, remaining = sum([portions[i] for i in movable]), surplus
        for i in movable:
            extra = min(reach - given[i], max(1, remaining * portions[i] // mass), surplus)
            given[i] = given[i] + extra
            surplus = surplus - extra
    return np.array([reach] + given)


def ragged(rng, amount, total, most, lean):
    if amount == 2:
        one = jax.random.randint(rng, (), max(1, total - most), min(most, total - 1) + 1)
        return jnp.stack([one, total - one])
    sizes = jnp.asarray(profile(amount, total, most, lean), jnp.int32)
    couples = (amount - 1) // 2
    source_of, taker = sizes[1:1 + 2 * couples:2], sizes[2:2 + 2 * couples:2]
    slack = jnp.minimum(source_of - 1, most - taker)
    shifted = jax.random.randint(jax.random.fold_in(rng, 1), (couples,), 0, 1 << 20) % (slack + 1)
    sizes = sizes.at[1:1 + 2 * couples:2].set(source_of - shifted).at[2:2 + 2 * couples:2].set(taker + shifted)
    return sizes[jax.random.permutation(jax.random.fold_in(rng, 2), amount)]


def scatter_about(stream_key, dims, scale, limit, pieces=(), kind=jnp.bfloat16):
    array = scale * jax.random.normal(stream_key, dims, jnp.float32)
    if pieces:
        array = array * block_scale(stream_key, dims, pieces, -0.22, 0.18)
    return jnp.clip(array, -limit, limit).astype(kind)


def setup_inputs(seed: int = 0) -> dict:
    key_list = jax.random.split(jax.random.key(seed), 10)
    hidden = draw_hidden(jax.random.fold_in(key_list[9], 71), 0)
    norm_gains = jnp.clip(1.0 + 0.1 * jax.random.normal(key_list[1], (LAYERS, D), jnp.float32), 0.5, 1.5).astype(jnp.bfloat16)
    w_query = scatter_about(key_list[2], (LAYERS, D, HQ * HD), D ** -0.5, 0.0625, ((1, 16), (2, 8)))
    w_key = scatter_about(key_list[3], (LAYERS, D, KVH * HD), (D // 4) ** -0.5, 0.125, ((1, 16), (2, 8)))
    w_value = scatter_about(key_list[4], (LAYERS, D, KVH * HD), (D // 4) ** -0.5, 0.125, ((1, 16), (2, 8)))
    w_out = scatter_about(key_list[5], (LAYERS, HQ * HD, D), (HQ * HD) ** -0.5, 0.0625, ((1, 8), (2, 16)))
    key_cache = scatter_about(key_list[6], (LAYERS, BATCH, KVH, CAP, HD), 1.5, 9.0, ((2, 8), (3, 16)))
    value_cache = scatter_about(key_list[7], (LAYERS, BATCH, KVH, CAP, HD), 1.0, 6.0, ((2, 8), (3, 16)))
    lengths = ragged(key_list[8], BATCH, BATCH * CAP // 2 + BATCH, CAP, 2).astype(jnp.int32)
    return dict(hidden=hidden, norm_gains=norm_gains, w_query=w_query, w_key=w_key, w_value=w_value, w_out=w_out, key_cache=key_cache, value_cache=value_cache, lengths=lengths)


mask_fill = -1e+30
norm_eps = 1e-05
rope_base = 500000.0

def rotate(vectors, positions):
    width = vectors.shape[-1]
    half_width = width // 2
    exponents = jnp.arange(half_width, dtype=jnp.float32) * (2.0 / width)
    frequency = jnp.exp(-exponents * math.log(rope_base))
    angles = positions.astype(jnp.float32)[:, None] * frequency[None, :]
    cosine = jnp.cos(angles)[:, None, :]
    sine_part = jnp.sin(angles)[:, None, :]
    first_half = vectors[..., :half_width]
    second_half = vectors[..., half_width:]
    return jnp.concatenate([first_half * cosine - second_half * sine_part, second_half * cosine + first_half * sine_part], axis=-1)

def reference(hidden, norm_gains, w_query, w_key, w_value, w_out, key_cache, value_cache, lengths):
    stream = hidden.astype(jnp.float32)
    group_size = HQ // KVH
    logit_multiplier = 1.0 / math.sqrt(HD)
    positions = jnp.arange(CAP, dtype=jnp.int32)
    usable = (positions[None, :] < lengths[:, None])[:, None, None, :]
    for layer_idx in range(LAYERS):
        reciprocal_value = lax.rsqrt(lax.optimization_barrier(jnp.sum(stream * stream, axis=1)) / D + norm_eps)
        scaled = (stream * norm_gains[layer_idx].astype(jnp.float32)).astype(jnp.bfloat16)
        raw_query = jnp.dot(scaled, w_query[layer_idx], preferred_element_type=jnp.float32)
        raw_key = jnp.dot(scaled, w_key[layer_idx], preferred_element_type=jnp.float32)
        raw_value = jnp.dot(scaled, w_value[layer_idx], preferred_element_type=jnp.float32)
        query = rotate((raw_query * reciprocal_value[:, None]).reshape(BATCH, HQ, HD), lengths).astype(jnp.bfloat16)
        fresh_lookup_vector = rotate((raw_key * reciprocal_value[:, None]).reshape(BATCH, KVH, HD), lengths).astype(jnp.bfloat16)
        new_value = (raw_value * reciprocal_value[:, None]).reshape(BATCH, KVH, HD).astype(jnp.bfloat16)
        shared_head_sets = query.reshape(BATCH, KVH, group_size, HD).astype(jnp.float32)
        scores = jnp.einsum('bkgd,bksd->bkgs', shared_head_sets, key_cache[layer_idx].astype(jnp.float32), precision=lax.Precision.HIGHEST) * logit_multiplier
        self_match_logit = jnp.einsum('uryj,urj->ury', shared_head_sets, fresh_lookup_vector.astype(jnp.float32), precision=lax.Precision.HIGHEST) * logit_multiplier
        masked = jnp.where(usable, scores, mask_fill)
        largest = jnp.maximum(lax.optimization_barrier(jnp.max(masked, axis=-1)), self_match_logit)
        attention_probabilities = jnp.where(usable, jnp.exp(masked - largest[..., None]), 0.0)
        fresh = jnp.exp(self_match_logit - largest)
        nearest_whole = lax.optimization_barrier(attention_probabilities.astype(jnp.bfloat16)).astype(jnp.float32)
        fresh_rounded = lax.optimization_barrier(fresh.astype(jnp.bfloat16)).astype(jnp.float32)
        numerator = jnp.einsum('bkgs,bksd->bkgd', nearest_whole, value_cache[layer_idx].astype(jnp.float32), precision=lax.Precision.HIGHEST)
        numerator = numerator + fresh_rounded[..., None] * new_value.astype(jnp.float32)[:, :, None, :]
        denominator = lax.optimization_barrier(jnp.sum(attention_probabilities, axis=-1)) + fresh
        context = (numerator / denominator[..., None]).reshape(BATCH, HQ * HD).astype(jnp.bfloat16)
        stream = stream + jnp.dot(context, w_out[layer_idx], preferred_element_type=jnp.float32)
    return stream
```

```python
import math

import jax
import jax.numpy as jnp
from jax import lax
from jax.sharding import Mesh
from jax.sharding import PartitionSpec as P

D = 8192
CTX = ("y", "x")

mask_fill = -1e30
norm_eps = 1e-05
rope_base = 500000.0

NEAR = ((0, 1), (1, 0), (2, 3), (3, 2))
WRAP = ((0, 3), (3, 0), (2, 1), (1, 2))
FAR = ((0, 2), (2, 0), (1, 3), (3, 1))


def exchange(shard, axis):
    return [shard] + [lax.ppermute(shard, axis, pairs) for pairs in (NEAR, WRAP, FAR)]


def ring_sum(shard, axis):
    own, near, wrap, far = exchange(shard, axis)
    return (own + near) + (wrap + far)


def rotate(vectors, cosine, sine):
    half = vectors.shape[-1] // 2
    u1, u2 = vectors[..., :half], vectors[..., half:]
    return jnp.concatenate([u1 * cosine - u2 * sine, u2 * cosine + u1 * sine], axis=-1)


def merge(shard, axis, batch, heads, width):
    shards = exchange(shard, axis)
    outs = [s[:, : heads * width].reshape(batch, heads, width) for s in shards]
    tops = [s[:, heads * width : heads * width + heads] for s in shards]
    sums = [s[:, heads * width + heads : heads * width + 2 * heads] for s in shards]
    top = jnp.maximum(jnp.maximum(tops[0], tops[1]), jnp.maximum(tops[2], tops[3]))
    factors = [jnp.exp(t - top) for t in tops]
    total = sum(f * s for f, s in zip(factors, sums))
    out = sum(f[..., None] * o for f, o in zip(factors, outs))
    return out, top, total


def pack(out, top, total):
    batch = out.shape[0]
    flat = out.reshape(batch, -1)
    heads = top.shape[1]
    pad = jnp.zeros((batch, 128 - 2 * heads), jnp.float32)
    return jnp.concatenate([flat, top, total, pad], axis=1)


def on_device(hidden, norm_gains, w_query, w_key, w_value, w_out, key_cache, value_cache, lengths):
    stream = hidden.astype(jnp.float32)
    batch = hidden.shape[0]
    width = key_cache.shape[4]
    location_total = key_cache.shape[3]
    q_cols = w_query.shape[2]
    heads = q_cols // width
    scale = 1.0 / math.sqrt(width)
    positions = lax.axis_index(CTX) * location_total + jnp.arange(location_total, dtype=jnp.int32)
    usable = (positions[None, :] < lengths[:, None])[:, None, :]
    exponents = jnp.arange(width // 2, dtype=jnp.float32) * (2.0 / width)
    frequency = jnp.exp(-exponents * math.log(rope_base))
    angles = lengths.astype(jnp.float32)[:, None] * frequency[None, :]
    cosine, sine = jnp.cos(angles)[:, None, :], jnp.sin(angles)[:, None, :]
    for layer in range(w_query.shape[0]):
        squares = jnp.sum(stream * stream, axis=1, keepdims=True)
        scaled = (stream * norm_gains[layer].astype(jnp.float32)).astype(jnp.bfloat16)
        parts = [
            jnp.dot(scaled, w[layer], preferred_element_type=jnp.float32)
            for w in (w_query, w_key, w_value)
        ]
        packed = jnp.concatenate(parts + [jnp.broadcast_to(squares, (batch, 128))], axis=1)
        packed = ring_sum(ring_sum(packed, "x"), "y")
        inverse = lax.rsqrt(packed[:, q_cols + 2 * width :][:, :1] / D + norm_eps)
        raw = (packed[:, : q_cols + 2 * width] * inverse).reshape(batch, heads + 2, width)
        rotated = rotate(raw[:, : heads + 1], cosine, sine).astype(jnp.bfloat16)
        query, new_key = rotated[:, :heads], rotated[:, heads]
        new_value = raw[:, heads + 1].astype(jnp.bfloat16)
        scores = (
            jnp.einsum(
                "bgd,bsd->bgs", query, key_cache[layer, :, 0], preferred_element_type=jnp.float32
            )
            * scale
        )
        masked = jnp.where(usable, scores, mask_fill)
        top = jnp.max(masked, axis=-1)
        weight = jnp.where(usable, jnp.exp(masked - top[..., None]), 0.0)
        total = jnp.sum(weight, axis=-1)
        out = jnp.einsum(
            "bgs,bsd->bgd",
            weight.astype(jnp.bfloat16),
            value_cache[layer, :, 0],
            preferred_element_type=jnp.float32,
        )
        out, top, total = merge(pack(out, top, total), "x", batch, heads, width)
        out, top, total = merge(pack(out, top, total), "y", batch, heads, width)
        own = jnp.einsum("bgd,bd->bg", query, new_key, preferred_element_type=jnp.float32) * scale
        largest = jnp.maximum(top, own)
        carried = jnp.exp(top - largest)
        fresh = jnp.exp(own - largest)
        fresh_rounded = fresh.astype(jnp.bfloat16).astype(jnp.float32)
        numerator = (
            out * carried[..., None] + fresh_rounded[..., None] * new_value.astype(jnp.float32)[:, None, :]
        )
        denominator = total * carried + fresh
        context = (numerator / denominator[..., None]).reshape(batch, q_cols).astype(jnp.bfloat16)
        head_part = jnp.dot(context, w_out[layer], preferred_element_type=jnp.float32)
        head_part = head_part + lax.ppermute(head_part, "core", ((0, 1), (1, 0)))
        stream = stream + ring_sum(head_part, "z")
    return stream


def solution(mesh):
    finer = Mesh(mesh.devices.reshape(4, 4, 4, 2), ("y", "x", "z", "core"))
    tp = ("z", "core")
    return jax.shard_map(
        on_device,
        mesh=finer,
        in_specs=(
            P(None, CTX),
            P(None, CTX),
            P(None, CTX, tp),
            P(None, CTX, tp),
            P(None, CTX, tp),
            P(None, tp, CTX),
            P(None, None, tp, CTX, None),
            P(None, None, tp, CTX, None),
            P(),
        ),
        out_specs=P(None, CTX),
        check_vma=False,
    )
```

```python
import functools
import math

import jax
import jax.numpy as jnp
from jax import lax
from jax.experimental import pallas as pl
from jax.experimental.pallas import tpu as pltpu
from jax.sharding import Mesh
from jax.sharding import PartitionSpec as P

D = 8192
CTX = ("y", "x")

mask_fill = -1e30
norm_eps = 1e-05
rope_base = 500000.0

NEAR = ((0, 1), (1, 0), (2, 3), (3, 2))
WRAP = ((0, 3), (3, 0), (2, 1), (1, 2))
FAR = ((0, 2), (2, 0), (1, 3), (3, 1))

LANES = 128


def exchange(shard, axis):
    return [shard] + [lax.ppermute(shard, axis, pairs) for pairs in (NEAR, WRAP, FAR)]


def total_of(parts):
    own, near, wrap, far = parts
    return (own + near) + (wrap + far)


def call(kernel, outs, *args):
    return pl.pallas_call(
        kernel,
        out_shape=outs,
        compiler_params=pltpu.CompilerParams(vmem_limit_bytes=16 * 1024 * 1024),
    )(*args)


def project_kernel(layer, *refs):
    *parts, gain_ref, wq_ref, wk_ref, wv_ref, packed_ref, stream_ref = refs
    stream = parts[0][...]
    if len(parts) > 1:
        stream = stream + total_of([p[...] for p in parts[1:]])
    stream_ref[...] = stream
    squares = jnp.sum(stream * stream, axis=1, keepdims=True)
    scaled = (stream * gain_ref[layer : layer + 1, :].astype(jnp.float32)).astype(jnp.bfloat16)
    q_cols = wq_ref.shape[2]
    packed_ref[:, :q_cols] = jnp.dot(scaled, wq_ref[layer], preferred_element_type=jnp.float32)
    packed_ref[:, q_cols : q_cols + LANES] = jnp.dot(
        scaled, wk_ref[layer], preferred_element_type=jnp.float32
    )
    packed_ref[:, q_cols + LANES : q_cols + 2 * LANES] = jnp.dot(
        scaled, wv_ref[layer], preferred_element_type=jnp.float32
    )
    packed_ref[:, q_cols + 2 * LANES :] = jnp.broadcast_to(squares, (stream.shape[0], LANES))


def attend_kernel(layer, scale, a_ref, b_ref, c_ref, d_ref, cos_ref, sin_ref, mask_ref, first_ref, key_ref, value_ref, out_ref):
    packed = total_of([a_ref[...], b_ref[...], c_ref[...], d_ref[...]])
    batch = packed.shape[0]
    heads = packed.shape[1] // LANES - 3
    inverse = lax.rsqrt(packed[:, (heads + 2) * LANES :] / D + norm_eps)
    cosine, sine = cos_ref[...], sin_ref[...]

    def column(i):
        return packed[:, i * LANES : (i + 1) * LANES] * inverse

    def rotated(i):
        u = column(i)
        return (u * cosine + pltpu.roll(u, LANES // 2, 1) * sine).astype(jnp.bfloat16)

    queries = [rotated(h) for h in range(heads)]
    new_key = rotated(heads).astype(jnp.float32)
    new_value = column(heads + 1).astype(jnp.bfloat16).astype(jnp.float32)
    query = jnp.concatenate(queries, axis=0)
    keys = key_ref[layer, :, 0].reshape(batch * LANES, LANES)
    values = value_ref[layer, :, 0].reshape(batch * LANES, LANES)
    scores = lax.dot_general(
        query, keys, (((1,), (1,)), ((), ())), preferred_element_type=jnp.float32
    )
    row = lax.broadcasted_iota(jnp.int32, (batch, LANES), 0)
    usable = mask_ref[...] > 0.0
    first = first_ref[...] > 0.0
    tops, sums, fresh_all, weights = [], [], [], []
    for h in range(heads):
        block = scores[h * batch : (h + 1) * batch, :]
        mine = block[:, :LANES]
        for b in range(1, batch):
            mine = jnp.where(row == b, block[:, b * LANES : (b + 1) * LANES], mine)
        mine = jnp.where(usable, mine * scale, mask_fill)
        own = jnp.sum(queries[h].astype(jnp.float32) * new_key, axis=1, keepdims=True) * scale
        own = jnp.where(first, own, mask_fill)
        top = jnp.maximum(jnp.max(mine, axis=1, keepdims=True), own)
        weight = jnp.where(usable, jnp.exp(mine - top), 0.0)
        fresh = jnp.where(first, jnp.exp(own - top), 0.0)
        sums.append(jnp.sum(weight, axis=1, keepdims=True) + fresh)
        tops.append(jnp.broadcast_to(top, (batch, LANES)))
        fresh_all.append(fresh.astype(jnp.bfloat16).astype(jnp.float32))
        weights.append(
            jnp.concatenate(
                [jnp.where(row == b, weight, 0.0).astype(jnp.bfloat16) for b in range(batch)], axis=1
            )
        )
    context = jnp.dot(jnp.concatenate(weights, axis=0), values, preferred_element_type=jnp.float32)
    lane = lax.broadcasted_iota(jnp.int32, (batch, LANES), 1)
    stats = jnp.zeros((batch, LANES), jnp.float32)
    for h in range(heads):
        out_ref[:, h * LANES : (h + 1) * LANES] = (
            context[h * batch : (h + 1) * batch, :] + fresh_all[h] * new_value
        )
        stats = jnp.where(lane == h, tops[h], stats)
        stats = jnp.where(lane == heads + h, sums[h], stats)
    out_ref[:, heads * LANES :] = stats


def merged(refs):
    shards = [r[...] for r in refs]
    heads = shards[0].shape[1] // LANES - 1
    batch = shards[0].shape[0]
    stats = [s[:, heads * LANES :] for s in shards]
    lane = lax.broadcasted_iota(jnp.int32, (batch, LANES), 1)
    is_top = lane < heads
    tops = [jnp.where(is_top, s, 0.0) for s in stats]
    top = jnp.maximum(jnp.maximum(tops[0], tops[1]), jnp.maximum(tops[2], tops[3]))
    factors = [jnp.exp(t - top) for t in tops]
    total = jnp.zeros((batch, LANES), jnp.float32)
    for f, s in zip(factors, stats):
        total = total + pltpu.roll(f, heads, 1) * s
    outs = []
    for h in range(heads):
        cols = slice(h * LANES, (h + 1) * LANES)
        outs.append(total_of([f[:, h : h + 1] * s[:, cols] for f, s in zip(factors, shards)]))
    return outs, jnp.where(is_top, top, total), total


def merge_kernel(a_ref, b_ref, c_ref, d_ref, out_ref):
    outs, stats, _ = merged((a_ref, b_ref, c_ref, d_ref))
    heads = len(outs)
    for h in range(heads):
        out_ref[:, h * LANES : (h + 1) * LANES] = outs[h]
    out_ref[:, heads * LANES :] = stats


def output_kernel(layer, a_ref, b_ref, c_ref, d_ref, wo_ref, out_ref):
    outs, _, total = merged((a_ref, b_ref, c_ref, d_ref))
    heads = len(outs)
    context = jnp.concatenate(
        [(outs[h] / total[:, heads + h : heads + h + 1]).astype(jnp.bfloat16) for h in range(heads)],
        axis=1,
    )
    out_ref[...] = jnp.dot(context, wo_ref[layer], preferred_element_type=jnp.float32)


def on_device(hidden, norm_gains, w_query, w_key, w_value, w_out, key_cache, value_cache, lengths):
    batch = hidden.shape[0]
    width = key_cache.shape[4]
    location_total = key_cache.shape[3]
    heads = w_query.shape[2] // width
    scale = 1.0 / math.sqrt(width)
    ctx_index = lax.axis_index(CTX)
    positions = ctx_index * location_total + jnp.arange(location_total, dtype=jnp.int32)
    usable = (positions[None, :] < lengths[:, None]).astype(jnp.float32)
    first = jnp.broadcast_to(ctx_index == 0, (batch, 1)).astype(jnp.float32)
    exponents = jnp.arange(width // 2, dtype=jnp.float32) * (2.0 / width)
    frequency = jnp.exp(-exponents * math.log(rope_base))
    angles = lengths.astype(jnp.float32)[:, None] * frequency[None, :]
    cosine, sine = jnp.cos(angles), jnp.sin(angles)
    cosine = jnp.concatenate([cosine, cosine], axis=1)
    sine = jnp.concatenate([-sine, sine], axis=1)

    f32 = jnp.float32
    packed_shape = jax.ShapeDtypeStruct((batch, (heads + 3) * width), f32)
    stream_shape = jax.ShapeDtypeStruct(hidden.shape, f32)
    mixed_shape = jax.ShapeDtypeStruct((batch, (heads + 1) * width), f32)
    parts = [hidden.astype(f32)]
    for layer in range(w_query.shape[0]):
        packed, stream = call(
            functools.partial(project_kernel, layer),
            (packed_shape, stream_shape),
            *parts, norm_gains, w_query, w_key, w_value,
        )
        packed = total_of(exchange(packed, "x"))
        mixed = call(
            functools.partial(attend_kernel, layer, scale),
            mixed_shape,
            *exchange(packed, "y"), cosine, sine, usable, first, key_cache, value_cache,
        )
        mixed = call(merge_kernel, mixed_shape, *exchange(mixed, "x"))
        head_part = call(
            functools.partial(output_kernel, layer), stream_shape, *exchange(mixed, "y"), w_out
        )
        head_part = head_part + lax.ppermute(head_part, "core", ((0, 1), (1, 0)))
        parts = [stream] + exchange(head_part, "z")
    return parts[0] + total_of(parts[1:])


def solution(mesh):
    finer = Mesh(mesh.devices.reshape(4, 4, 4, 2), ("y", "x", "z", "core"))
    tp = ("z", "core")
    return jax.shard_map(
        on_device,
        mesh=finer,
        in_specs=(
            P(None, CTX),
            P(None, CTX),
            P(None, CTX, tp),
            P(None, CTX, tp),
            P(None, CTX, tp),
            P(None, tp, CTX),
            P(None, None, tp, CTX, None),
            P(None, None, tp, CTX, None),
            P(),
        ),
        out_specs=P(None, CTX),
        check_vma=False,
    )
```

```python
import functools
import math

import jax
import jax.numpy as jnp
from jax import lax
from jax.experimental import pallas as pl
from jax.experimental.pallas import tpu as pltpu
from jax.sharding import Mesh
from jax.sharding import PartitionSpec as P

D = 8192
CTX = ("y", "x")

mask_fill = -1e30
norm_eps = 1e-05
rope_base = 500000.0

NEAR = ((0, 1), (1, 0), (2, 3), (3, 2))
WRAP = ((0, 3), (3, 0), (2, 1), (1, 2))
FAR = ((0, 2), (2, 0), (1, 3), (3, 1))

LANES = 128


def exchange(shard, axis):
    return [shard] + [lax.ppermute(shard, axis, pairs) for pairs in (NEAR, WRAP, FAR)]


def total_of(parts):
    own, near, wrap, far = parts
    return (own + near) + (wrap + far)


def sum_kernel(*refs):
    *parts, out_ref = refs
    if len(parts) == 2:
        out_ref[...] = parts[0][...] + parts[1][...]
    elif len(parts) == 4:
        out_ref[...] = total_of([p[...] for p in parts])
    else:
        out_ref[...] = parts[0][...] + total_of([p[...] for p in parts[1:]])


def call(kernel, outs, *args, **kwargs):
    return pl.pallas_call(
        kernel,
        out_shape=outs,
        compiler_params=pltpu.CompilerParams(vmem_limit_bytes=16 * 1024 * 1024),
        **kwargs,
    )(*args)


def like(array):
    return jax.ShapeDtypeStruct(array.shape, array.dtype)


def first_project(outs, *args):
    scratch = [pltpu.VMEM(a.shape[:-2] and (1,) + a.shape[1:] or a.shape, a.dtype) for a in args]
    hbm = pl.BlockSpec(memory_space=pltpu.MemorySpace.HBM)
    return call(
        first_project_kernel,
        outs,
        *[in_hbm(a) for a in args],
        in_specs=[hbm] * len(args),
        scratch_shapes=scratch + [pltpu.SemaphoreType.DMA((len(args),))],
    )


def in_hbm(array):
    return pltpu.with_memory_space_constraint(array, pltpu.MemorySpace.HBM)


def fetch_kernel(weight_hbm, after_hbm, out_ref, sem):
    copy = pltpu.make_async_copy(weight_hbm.at[0:1], out_ref, sem)
    copy.start()
    copy.wait()


def fetch_first(weight, after):
    hbm = pl.BlockSpec(memory_space=pltpu.MemorySpace.HBM)
    anywhere = pl.BlockSpec(memory_space=pl.ANY)
    return call(
        fetch_kernel,
        jax.ShapeDtypeStruct((1,) + weight.shape[1:], weight.dtype),
        in_hbm(weight),
        after,
        in_specs=[hbm, anywhere],
        out_specs=pl.BlockSpec(memory_space=pltpu.VMEM),
        scratch_shapes=[pltpu.SemaphoreType.DMA(())],
    )


def sum_of(*parts):
    return call(sum_kernel, like(parts[0]), *parts)


def across(shard):
    pairs = []
    for ring in (NEAR, WRAP, FAR):
        pairs.append([(2 * s + c, 2 * t + 1 - c) for s, t in ring for c in range(2)])
    return [shard] + [lax.ppermute(shard, ("z", "core"), p) for p in pairs]


def first_project_kernel(
    hidden_hbm, gain_hbm, wq_hbm, wk_hbm, wv_hbm, packed_ref, stream_ref,
    hidden_ref, gain_ref, wq_ref, wk_ref, wv_ref, sems,
):
    moves = (
        (hidden_hbm, hidden_ref),
        (gain_hbm, gain_ref),
        (wk_hbm.at[0:1], wk_ref),
        (wv_hbm.at[0:1], wv_ref),
        (wq_hbm.at[0:1], wq_ref),
    )
    copies = [pltpu.make_async_copy(s, d, sems.at[i]) for i, (s, d) in enumerate(moves)]
    for copy in copies:
        copy.start()
    for copy in copies:
        copy.wait()
    project(0, hidden_ref[...].astype(jnp.float32), gain_ref, wq_ref, wk_ref, wv_ref, packed_ref, stream_ref)


def project_kernel(layer, *refs):
    *parts, gain_ref, wq_ref, wk_ref, wv_ref, packed_ref, stream_ref = refs
    stream = parts[0][...] + total_of([p[...] for p in parts[1:]])
    project(layer, stream, gain_ref, wq_ref, wk_ref, wv_ref, packed_ref, stream_ref)


def project(layer, stream, gain_ref, wq_ref, wk_ref, wv_ref, packed_ref, stream_ref):
    stream_ref[...] = stream
    squares = jnp.sum(stream * stream, axis=1, keepdims=True)
    scaled = (stream * gain_ref[layer : layer + 1, :].astype(jnp.float32)).astype(jnp.bfloat16)
    q_cols = wq_ref.shape[2]
    packed_ref[:, :q_cols] = jnp.dot(scaled, wq_ref[layer], preferred_element_type=jnp.float32)
    packed_ref[:, q_cols : q_cols + LANES] = jnp.dot(
        scaled, wk_ref[layer], preferred_element_type=jnp.float32
    )
    packed_ref[:, q_cols + LANES : q_cols + 2 * LANES] = jnp.dot(
        scaled, wv_ref[layer], preferred_element_type=jnp.float32
    )
    packed_ref[:, q_cols + 2 * LANES :] = jnp.broadcast_to(squares, (stream.shape[0], LANES))


def attend_kernel(layer, scale, a_ref, b_ref, c_ref, d_ref, cos_ref, sin_ref, mask_ref, first_ref, key_ref, value_ref, out_ref):
    packed = total_of([a_ref[...], b_ref[...], c_ref[...], d_ref[...]])
    batch = packed.shape[0]
    heads = packed.shape[1] // LANES - 3
    inverse = lax.rsqrt(packed[:, (heads + 2) * LANES :] / D + norm_eps)
    cosine, sine = cos_ref[...], sin_ref[...]

    def column(i):
        return packed[:, i * LANES : (i + 1) * LANES] * inverse

    def rotated(i):
        u = column(i)
        return (u * cosine + pltpu.roll(u, LANES // 2, 1) * sine).astype(jnp.bfloat16)

    queries = [rotated(h) for h in range(heads)]
    new_key = rotated(heads).astype(jnp.float32)
    new_value = column(heads + 1).astype(jnp.bfloat16).astype(jnp.float32)
    query = jnp.concatenate(queries, axis=0)
    keys = key_ref[layer, :, 0].reshape(batch * LANES, LANES)
    values = value_ref[layer, :, 0].reshape(batch * LANES, LANES)
    scores = lax.dot_general(
        query, keys, (((1,), (1,)), ((), ())), preferred_element_type=jnp.float32
    )
    row = lax.broadcasted_iota(jnp.int32, (batch, LANES), 0)
    usable = mask_ref[...] > 0.0
    first = first_ref[...] > 0.0
    tops, sums, fresh_all, weights = [], [], [], []
    for h in range(heads):
        block = scores[h * batch : (h + 1) * batch, :]
        mine = block[:, :LANES]
        for b in range(1, batch):
            mine = jnp.where(row == b, block[:, b * LANES : (b + 1) * LANES], mine)
        mine = jnp.where(usable, mine * scale, mask_fill)
        own = jnp.sum(queries[h].astype(jnp.float32) * new_key, axis=1, keepdims=True) * scale
        own = jnp.where(first, own, mask_fill)
        top = jnp.maximum(jnp.max(mine, axis=1, keepdims=True), own)
        weight = jnp.where(usable, jnp.exp(mine - top), 0.0)
        fresh = jnp.where(first, jnp.exp(own - top), 0.0)
        sums.append(jnp.sum(weight, axis=1, keepdims=True) + fresh)
        tops.append(jnp.broadcast_to(top, (batch, LANES)))
        fresh_all.append(fresh.astype(jnp.bfloat16).astype(jnp.float32))
        weights.append(
            jnp.concatenate(
                [jnp.where(row == b, weight, 0.0).astype(jnp.bfloat16) for b in range(batch)], axis=1
            )
        )
    context = jnp.dot(jnp.concatenate(weights, axis=0), values, preferred_element_type=jnp.float32)
    lane = lax.broadcasted_iota(jnp.int32, (batch, LANES), 1)
    stats = jnp.zeros((batch, LANES), jnp.float32)
    for h in range(heads):
        out_ref[:, h * LANES : (h + 1) * LANES] = (
            context[h * batch : (h + 1) * batch, :] + fresh_all[h] * new_value
        )
        stats = jnp.where(lane == h, tops[h], stats)
        stats = jnp.where(lane == heads + h, sums[h], stats)
    out_ref[:, heads * LANES :] = stats


def merged(refs):
    shards = [r[...] for r in refs]
    heads = shards[0].shape[1] // LANES - 1
    batch = shards[0].shape[0]
    stats = [s[:, heads * LANES :] for s in shards]
    lane = lax.broadcasted_iota(jnp.int32, (batch, LANES), 1)
    is_top = lane < heads
    tops = [jnp.where(is_top, s, 0.0) for s in stats]
    top = jnp.maximum(jnp.maximum(tops[0], tops[1]), jnp.maximum(tops[2], tops[3]))
    factors = [jnp.exp(t - top) for t in tops]
    total = jnp.zeros((batch, LANES), jnp.float32)
    for f, s in zip(factors, stats):
        total = total + pltpu.roll(f, heads, 1) * s
    outs = []
    for h in range(heads):
        cols = slice(h * LANES, (h + 1) * LANES)
        outs.append(total_of([f[:, h : h + 1] * s[:, cols] for f, s in zip(factors, shards)]))
    return outs, jnp.where(is_top, top, total), total


def merge_kernel(a_ref, b_ref, c_ref, d_ref, out_ref):
    outs, stats, _ = merged((a_ref, b_ref, c_ref, d_ref))
    heads = len(outs)
    for h in range(heads):
        out_ref[:, h * LANES : (h + 1) * LANES] = outs[h]
    out_ref[:, heads * LANES :] = stats


def output_kernel(layer, a_ref, b_ref, c_ref, d_ref, wo_ref, out_ref):
    outs, _, total = merged((a_ref, b_ref, c_ref, d_ref))
    heads = len(outs)
    context = jnp.concatenate(
        [(outs[h] / total[:, heads + h : heads + h + 1]).astype(jnp.bfloat16) for h in range(heads)],
        axis=1,
    )
    out_ref[...] = jnp.dot(context, wo_ref[layer], preferred_element_type=jnp.float32)


def on_device(hidden, norm_gains, w_query, w_key, w_value, w_out, key_cache, value_cache, lengths):
    batch = hidden.shape[0]
    width = key_cache.shape[4]
    location_total = key_cache.shape[3]
    heads = w_query.shape[2] // width
    scale = 1.0 / math.sqrt(width)
    ctx_index = lax.axis_index(CTX)
    positions = ctx_index * location_total + jnp.arange(location_total, dtype=jnp.int32)
    usable = (positions[None, :] < lengths[:, None]).astype(jnp.float32)
    first = jnp.broadcast_to(ctx_index == 0, (batch, 1)).astype(jnp.float32)
    exponents = jnp.arange(width // 2, dtype=jnp.float32) * (2.0 / width)
    frequency = jnp.exp(-exponents * math.log(rope_base))
    angles = lengths.astype(jnp.float32)[:, None] * frequency[None, :]
    cosine, sine = jnp.cos(angles), jnp.sin(angles)
    cosine = jnp.concatenate([cosine, cosine], axis=1)
    sine = jnp.concatenate([-sine, sine], axis=1)

    f32 = jnp.float32
    packed_shape = jax.ShapeDtypeStruct((batch, (heads + 3) * width), f32)
    stream_shape = jax.ShapeDtypeStruct(hidden.shape, f32)
    mixed_shape = jax.ShapeDtypeStruct((batch, (heads + 1) * width), f32)
    weights = (norm_gains, w_query, w_key, w_value)
    parts = None
    for layer in range(w_query.shape[0]):
        if layer == 0:
            packed, stream = first_project((packed_shape, stream_shape), hidden, *weights)
            w_out_first = fetch_first(w_out, packed)
        else:
            packed, stream = call(
                functools.partial(project_kernel, layer), (packed_shape, stream_shape), *parts, *weights
            )
        packed = sum_of(*exchange(packed, "x"))
        mixed = call(
            functools.partial(attend_kernel, layer, scale),
            mixed_shape,
            *exchange(packed, "y"), cosine, sine, usable, first, key_cache, value_cache,
        )
        mixed = call(merge_kernel, mixed_shape, *exchange(mixed, "x"))
        head_part = call(
            functools.partial(output_kernel, layer),
            stream_shape,
            *exchange(mixed, "y"),
            w_out if layer else w_out_first,
        )
        head_part = sum_of(head_part, lax.ppermute(head_part, "core", ((0, 1), (1, 0))))
        parts = [stream] + across(head_part)
    return sum_of(*parts)


def solution(mesh):
    finer = Mesh(mesh.devices.reshape(4, 4, 4, 2), ("y", "x", "z", "core"))
    tp = ("z", "core")
    return jax.shard_map(
        on_device,
        mesh=finer,
        in_specs=(
            P(None, CTX),
            P(None, CTX),
            P(None, CTX, tp),
            P(None, CTX, tp),
            P(None, CTX, tp),
            P(None, tp, CTX),
            P(None, None, tp, CTX, None),
            P(None, None, tp, CTX, None),
            P(),
        ),
        out_specs=P(None, CTX),
        check_vma=False,
    )
```

```python
import functools
import math

import jax
import jax.numpy as jnp
from jax import lax
from jax.experimental import pallas as pl
from jax.experimental.pallas import tpu as pltpu
from jax.sharding import Mesh
from jax.sharding import PartitionSpec as P

D = 8192
CTX = ("y", "x")

mask_fill = -1e30
norm_eps = 1e-05
rope_base = 500000.0

NEAR = ((0, 1), (1, 0), (2, 3), (3, 2))
WRAP = ((0, 3), (3, 0), (2, 1), (1, 2))
FAR = ((0, 2), (2, 0), (1, 3), (3, 1))

LANES = 128


RINGS = {"N": NEAR, "W": WRAP, "F": FAR}
CROSSED = "F"


def crossed(pairs):
    return [(2 * s + c, 2 * t + 1 - c) for s, t in pairs for c in range(2)]


def exchange(shard, axis):
    got = {}
    for name in "NWF":
        if name in CROSSED:
            got[name] = lax.ppermute(shard, (axis, "core"), crossed(RINGS[name]))
        else:
            got[name] = lax.ppermute(shard, axis, RINGS[name])
    for name in CROSSED:
        got[name] = lax.ppermute(got[name], "core", ((0, 1), (1, 0)))
    return [shard, got["N"], got["W"], got["F"]]


def total_of(parts):
    own, near, wrap, far = parts
    return (own + near) + (wrap + far)


def sum_kernel(*refs):
    *parts, out_ref = refs
    if len(parts) == 2:
        out_ref[...] = parts[0][...] + parts[1][...]
    elif len(parts) == 4:
        out_ref[...] = total_of([p[...] for p in parts])
    else:
        out_ref[...] = parts[0][...] + total_of([p[...] for p in parts[1:]])


def call(kernel, outs, *args, **kwargs):
    return pl.pallas_call(
        kernel,
        out_shape=outs,
        compiler_params=pltpu.CompilerParams(vmem_limit_bytes=16 * 1024 * 1024),
        **kwargs,
    )(*args)


def like(array):
    return jax.ShapeDtypeStruct(array.shape, array.dtype)


def first_project(outs, *args):
    scratch = [pltpu.VMEM(a.shape[:-2] and (1,) + a.shape[1:] or a.shape, a.dtype) for a in args]
    hbm = pl.BlockSpec(memory_space=pltpu.MemorySpace.HBM)
    return call(
        first_project_kernel,
        outs,
        *[in_hbm(a) for a in args],
        in_specs=[hbm] * len(args),
        scratch_shapes=scratch + [pltpu.SemaphoreType.DMA((len(args),))],
    )


def in_hbm(array):
    return pltpu.with_memory_space_constraint(array, pltpu.MemorySpace.HBM)


def fetch_kernel(weight_hbm, after_hbm, out_ref, sem):
    copy = pltpu.make_async_copy(weight_hbm.at[0:1], out_ref, sem)
    copy.start()
    copy.wait()


def fetch_first(weight, after):
    hbm = pl.BlockSpec(memory_space=pltpu.MemorySpace.HBM)
    anywhere = pl.BlockSpec(memory_space=pl.ANY)
    return call(
        fetch_kernel,
        jax.ShapeDtypeStruct((1,) + weight.shape[1:], weight.dtype),
        in_hbm(weight),
        after,
        in_specs=[hbm, anywhere],
        out_specs=pl.BlockSpec(memory_space=pltpu.VMEM),
        scratch_shapes=[pltpu.SemaphoreType.DMA(())],
    )


def sum_of(*parts):
    return call(sum_kernel, like(parts[0]), *parts)


def across(shard):
    pairs = []
    for ring in (NEAR, WRAP, FAR):
        pairs.append([(2 * s + c, 2 * t + 1 - c) for s, t in ring for c in range(2)])
    return [shard] + [lax.ppermute(shard, ("z", "core"), p) for p in pairs]


def first_project_kernel(
    hidden_hbm, gain_hbm, wq_hbm, wk_hbm, wv_hbm, packed_ref, stream_ref,
    hidden_ref, gain_ref, wq_ref, wk_ref, wv_ref, sems,
):
    moves = (
        (hidden_hbm, hidden_ref),
        (gain_hbm, gain_ref),
        (wk_hbm.at[0:1], wk_ref),
        (wv_hbm.at[0:1], wv_ref),
        (wq_hbm.at[0:1], wq_ref),
    )
    copies = [pltpu.make_async_copy(s, d, sems.at[i]) for i, (s, d) in enumerate(moves)]
    for copy in copies:
        copy.start()
    for copy in copies:
        copy.wait()
    project(0, hidden_ref[...].astype(jnp.float32), gain_ref, wq_ref, wk_ref, wv_ref, packed_ref, stream_ref)


def project_kernel(layer, *refs):
    *parts, gain_ref, wq_ref, wk_ref, wv_ref, packed_ref, stream_ref = refs
    stream = parts[0][...] + total_of([p[...] for p in parts[1:]])
    project(layer, stream, gain_ref, wq_ref, wk_ref, wv_ref, packed_ref, stream_ref)


def project(layer, stream, gain_ref, wq_ref, wk_ref, wv_ref, packed_ref, stream_ref):
    stream_ref[...] = stream
    squares = jnp.sum(stream * stream, axis=1, keepdims=True)
    scaled = (stream * gain_ref[layer : layer + 1, :].astype(jnp.float32)).astype(jnp.bfloat16)
    q_cols = wq_ref.shape[2]
    packed_ref[:, :q_cols] = jnp.dot(scaled, wq_ref[layer], preferred_element_type=jnp.float32)
    packed_ref[:, q_cols : q_cols + LANES] = jnp.dot(
        scaled, wk_ref[layer], preferred_element_type=jnp.float32
    )
    packed_ref[:, q_cols + LANES : q_cols + 2 * LANES] = jnp.dot(
        scaled, wv_ref[layer], preferred_element_type=jnp.float32
    )
    packed_ref[:, q_cols + 2 * LANES :] = jnp.broadcast_to(squares, (stream.shape[0], LANES))


def attend_kernel(layer, scale, a_ref, b_ref, c_ref, d_ref, cos_ref, sin_ref, mask_ref, first_ref, key_ref, value_ref, out_ref):
    packed = total_of([a_ref[...], b_ref[...], c_ref[...], d_ref[...]])
    batch = packed.shape[0]
    heads = packed.shape[1] // LANES - 3
    inverse = lax.rsqrt(packed[:, (heads + 2) * LANES :] / D + norm_eps)
    cosine, sine = cos_ref[...], sin_ref[...]

    def column(i):
        return packed[:, i * LANES : (i + 1) * LANES] * inverse

    def rotated(i):
        u = column(i)
        return (u * cosine + pltpu.roll(u, LANES // 2, 1) * sine).astype(jnp.bfloat16)

    queries = [rotated(h) for h in range(heads)]
    new_key = rotated(heads).astype(jnp.float32)
    new_value = column(heads + 1).astype(jnp.bfloat16).astype(jnp.float32)
    query = jnp.concatenate(queries, axis=0)
    keys = key_ref[layer, :, 0].reshape(batch * LANES, LANES)
    values = value_ref[layer, :, 0].reshape(batch * LANES, LANES)
    scores = lax.dot_general(
        query, keys, (((1,), (1,)), ((), ())), preferred_element_type=jnp.float32
    )
    row = lax.broadcasted_iota(jnp.int32, (batch, LANES), 0)
    usable = mask_ref[...] > 0.0
    first = first_ref[...] > 0.0
    tops, sums, fresh_all, weights = [], [], [], []
    for h in range(heads):
        block = scores[h * batch : (h + 1) * batch, :]
        mine = block[:, :LANES]
        for b in range(1, batch):
            mine = jnp.where(row == b, block[:, b * LANES : (b + 1) * LANES], mine)
        mine = jnp.where(usable, mine * scale, mask_fill)
        own = jnp.sum(queries[h].astype(jnp.float32) * new_key, axis=1, keepdims=True) * scale
        own = jnp.where(first, own, mask_fill)
        top = jnp.maximum(jnp.max(mine, axis=1, keepdims=True), own)
        weight = jnp.where(usable, jnp.exp(mine - top), 0.0)
        fresh = jnp.where(first, jnp.exp(own - top), 0.0)
        sums.append(jnp.sum(weight, axis=1, keepdims=True) + fresh)
        tops.append(jnp.broadcast_to(top, (batch, LANES)))
        fresh_all.append(fresh.astype(jnp.bfloat16).astype(jnp.float32))
        weights.append(
            jnp.concatenate(
                [jnp.where(row == b, weight, 0.0).astype(jnp.bfloat16) for b in range(batch)], axis=1
            )
        )
    context = jnp.dot(jnp.concatenate(weights, axis=0), values, preferred_element_type=jnp.float32)
    lane = lax.broadcasted_iota(jnp.int32, (batch, LANES), 1)
    stats = jnp.zeros((batch, LANES), jnp.float32)
    for h in range(heads):
        out_ref[:, h * LANES : (h + 1) * LANES] = (
            context[h * batch : (h + 1) * batch, :] + fresh_all[h] * new_value
        )
        stats = jnp.where(lane == h, tops[h], stats)
        stats = jnp.where(lane == heads + h, sums[h], stats)
    out_ref[:, heads * LANES :] = stats


def merged(refs):
    shards = [r[...] for r in refs]
    heads = shards[0].shape[1] // LANES - 1
    batch = shards[0].shape[0]
    stats = [s[:, heads * LANES :] for s in shards]
    lane = lax.broadcasted_iota(jnp.int32, (batch, LANES), 1)
    is_top = lane < heads
    tops = [jnp.where(is_top, s, 0.0) for s in stats]
    top = jnp.maximum(jnp.maximum(tops[0], tops[1]), jnp.maximum(tops[2], tops[3]))
    factors = [jnp.exp(t - top) for t in tops]
    total = jnp.zeros((batch, LANES), jnp.float32)
    for f, s in zip(factors, stats):
        total = total + pltpu.roll(f, heads, 1) * s
    outs = []
    for h in range(heads):
        cols = slice(h * LANES, (h + 1) * LANES)
        outs.append(total_of([f[:, h : h + 1] * s[:, cols] for f, s in zip(factors, shards)]))
    return outs, jnp.where(is_top, top, total), total


def merge_kernel(a_ref, b_ref, c_ref, d_ref, out_ref):
    outs, stats, _ = merged((a_ref, b_ref, c_ref, d_ref))
    heads = len(outs)
    for h in range(heads):
        out_ref[:, h * LANES : (h + 1) * LANES] = outs[h]
    out_ref[:, heads * LANES :] = stats


def output_kernel(layer, a_ref, b_ref, c_ref, d_ref, wo_ref, out_ref):
    outs, _, total = merged((a_ref, b_ref, c_ref, d_ref))
    heads = len(outs)
    context = jnp.concatenate(
        [(outs[h] / total[:, heads + h : heads + h + 1]).astype(jnp.bfloat16) for h in range(heads)],
        axis=1,
    )
    out_ref[...] = jnp.dot(context, wo_ref[layer], preferred_element_type=jnp.float32)


def on_device(hidden, norm_gains, w_query, w_key, w_value, w_out, key_cache, value_cache, lengths):
    batch = hidden.shape[0]
    width = key_cache.shape[4]
    location_total = key_cache.shape[3]
    heads = w_query.shape[2] // width
    scale = 1.0 / math.sqrt(width)
    ctx_index = lax.axis_index(CTX)
    positions = ctx_index * location_total + jnp.arange(location_total, dtype=jnp.int32)
    usable = (positions[None, :] < lengths[:, None]).astype(jnp.float32)
    first = jnp.broadcast_to(ctx_index == 0, (batch, 1)).astype(jnp.float32)
    exponents = jnp.arange(width // 2, dtype=jnp.float32) * (2.0 / width)
    frequency = jnp.exp(-exponents * math.log(rope_base))
    angles = lengths.astype(jnp.float32)[:, None] * frequency[None, :]
    cosine, sine = jnp.cos(angles), jnp.sin(angles)
    cosine = jnp.concatenate([cosine, cosine], axis=1)
    sine = jnp.concatenate([-sine, sine], axis=1)

    f32 = jnp.float32
    packed_shape = jax.ShapeDtypeStruct((batch, (heads + 3) * width), f32)
    stream_shape = jax.ShapeDtypeStruct(hidden.shape, f32)
    mixed_shape = jax.ShapeDtypeStruct((batch, (heads + 1) * width), f32)
    weights = (norm_gains, w_query, w_key, w_value)
    parts = None
    for layer in range(w_query.shape[0]):
        if layer == 0:
            packed, stream = first_project((packed_shape, stream_shape), hidden, *weights)
            w_out_first = fetch_first(w_out, packed)
        else:
            packed, stream = call(
                functools.partial(project_kernel, layer), (packed_shape, stream_shape), *parts, *weights
            )
        packed = sum_of(*exchange(packed, "x"))
        mixed = call(
            functools.partial(attend_kernel, layer, scale),
            mixed_shape,
            *exchange(packed, "y"), cosine, sine, usable, first, key_cache, value_cache,
        )
        mixed = call(merge_kernel, mixed_shape, *exchange(mixed, "x"))
        head_part = call(
            functools.partial(output_kernel, layer),
            stream_shape,
            *exchange(mixed, "y"),
            w_out if layer else w_out_first,
        )
        head_part = sum_of(head_part, lax.ppermute(head_part, "core", ((0, 1), (1, 0))))
        parts = [stream] + across(head_part)
    return sum_of(*parts)


def solution(mesh):
    finer = Mesh(mesh.devices.reshape(4, 4, 4, 2), ("y", "x", "z", "core"))
    tp = ("z", "core")
    return jax.shard_map(
        on_device,
        mesh=finer,
        in_specs=(
            P(None, CTX),
            P(None, CTX),
            P(None, CTX, tp),
            P(None, CTX, tp),
            P(None, CTX, tp),
            P(None, tp, CTX),
            P(None, None, tp, CTX, None),
            P(None, None, tp, CTX, None),
            P(),
        ),
        out_specs=P(None, CTX),
        check_vma=False,
    )
```

```python
import functools
import math

import jax
import jax.numpy as jnp
from jax import lax
from jax.experimental import pallas as pl
from jax.experimental.pallas import tpu as pltpu
from jax.sharding import Mesh
from jax.sharding import PartitionSpec as P

D = 8192
CTX = ("y", "x")

mask_fill = -1e30
norm_eps = 1e-05
rope_base = 500000.0

NEAR = ((0, 1), (1, 0), (2, 3), (3, 2))
WRAP = ((0, 3), (3, 0), (2, 1), (1, 2))
FAR = ((0, 2), (2, 0), (1, 3), (3, 1))

LANES = 128


RINGS = {"N": NEAR, "W": WRAP, "F": FAR}
CROSSED = "F"


def crossed(pairs):
    return [(2 * s + c, 2 * t + 1 - c) for s, t in pairs for c in range(2)]


def exchange(shard, axis):
    got = {}
    for name in "WNF":
        if name in CROSSED:
            got[name] = lax.ppermute(shard, (axis, "core"), crossed(RINGS[name]))
        else:
            got[name] = lax.ppermute(shard, axis, RINGS[name])
    for name in CROSSED:
        got[name] = lax.ppermute(got[name], "core", ((0, 1), (1, 0)))
    return [shard, got["N"], got["W"], got["F"]]


def total_of(parts):
    own, near, wrap, far = parts
    return (own + near) + (wrap + far)


def sum_kernel(*refs):
    *parts, out_ref = refs
    if len(parts) == 2:
        out_ref[...] = parts[0][...] + parts[1][...]
    elif len(parts) == 4:
        out_ref[...] = total_of([p[...] for p in parts])
    else:
        out_ref[...] = parts[0][...] + total_of([p[...] for p in parts[1:]])


def call(kernel, outs, *args, **kwargs):
    return pl.pallas_call(
        kernel,
        out_shape=outs,
        compiler_params=pltpu.CompilerParams(vmem_limit_bytes=16 * 1024 * 1024),
        **kwargs,
    )(*args)


def like(array):
    return jax.ShapeDtypeStruct(array.shape, array.dtype)


def first_project(outs, *args):
    scratch = [pltpu.VMEM(a.shape[:-2] and (1,) + a.shape[1:] or a.shape, a.dtype) for a in args]
    hbm = pl.BlockSpec(memory_space=pltpu.MemorySpace.HBM)
    return call(
        first_project_kernel,
        outs,
        *[in_hbm(a) for a in args],
        in_specs=[hbm] * len(args),
        scratch_shapes=scratch + [pltpu.SemaphoreType.DMA((len(args),))],
    )


def in_hbm(array):
    return pltpu.with_memory_space_constraint(array, pltpu.MemorySpace.HBM)


def fetch_kernel(weight_hbm, after_hbm, out_ref, sem):
    copy = pltpu.make_async_copy(weight_hbm.at[0:1], out_ref, sem)
    copy.start()
    copy.wait()


def fetch_first(weight, after):
    hbm = pl.BlockSpec(memory_space=pltpu.MemorySpace.HBM)
    anywhere = pl.BlockSpec(memory_space=pl.ANY)
    return call(
        fetch_kernel,
        jax.ShapeDtypeStruct((1,) + weight.shape[1:], weight.dtype),
        in_hbm(weight),
        after,
        in_specs=[hbm, anywhere],
        out_specs=pl.BlockSpec(memory_space=pltpu.VMEM),
        scratch_shapes=[pltpu.SemaphoreType.DMA(())],
    )


def sum_of(*parts):
    return call(sum_kernel, like(parts[0]), *parts)


def across(shard):
    pairs = []
    for ring in (NEAR, WRAP, FAR):
        pairs.append([(2 * s + c, 2 * t + 1 - c) for s, t in ring for c in range(2)])
    return [shard] + [lax.ppermute(shard, ("z", "core"), p) for p in pairs]


def first_project_kernel(
    hidden_hbm, gain_hbm, wq_hbm, wk_hbm, wv_hbm, packed_ref, stream_ref,
    hidden_ref, gain_ref, wq_ref, wk_ref, wv_ref, sems,
):
    moves = (
        (hidden_hbm, hidden_ref),
        (gain_hbm, gain_ref),
        (wk_hbm.at[0:1], wk_ref),
        (wv_hbm.at[0:1], wv_ref),
        (wq_hbm.at[0:1], wq_ref),
    )
    copies = [pltpu.make_async_copy(s, d, sems.at[i]) for i, (s, d) in enumerate(moves)]
    for copy in reversed(copies):
        copy.start()
    for copy in copies[:2]:
        copy.wait()
    stream = hidden_ref[...].astype(jnp.float32)
    project(0, stream, gain_ref, wq_ref, wk_ref, wv_ref, packed_ref, stream_ref, copies[2:])


def project_kernel(layer, *refs):
    *parts, gain_ref, wq_ref, wk_ref, wv_ref, packed_ref, stream_ref = refs
    stream = parts[0][...] + total_of([p[...] for p in parts[1:]])
    project(layer, stream, gain_ref, wq_ref, wk_ref, wv_ref, packed_ref, stream_ref)


def project(
    layer, stream, gain_ref, wq_ref, wk_ref, wv_ref, packed_ref, stream_ref, arrivals=()
):
    stream_ref[...] = stream
    squares = jnp.sum(stream * stream, axis=1, keepdims=True)
    scaled = (stream * gain_ref[layer : layer + 1, :].astype(jnp.float32)).astype(jnp.bfloat16)
    q_cols = wq_ref.shape[2]
    for arrival in arrivals[:2]:
        arrival.wait()
    packed_ref[:, q_cols : q_cols + LANES] = jnp.dot(
        scaled, wk_ref[layer], preferred_element_type=jnp.float32
    )
    packed_ref[:, q_cols + LANES : q_cols + 2 * LANES] = jnp.dot(
        scaled, wv_ref[layer], preferred_element_type=jnp.float32
    )
    packed_ref[:, q_cols + 2 * LANES :] = jnp.broadcast_to(squares, (stream.shape[0], LANES))
    for arrival in arrivals[2:]:
        arrival.wait()
    packed_ref[:, :q_cols] = jnp.dot(scaled, wq_ref[layer], preferred_element_type=jnp.float32)


def attend_kernel(layer, scale, a_ref, b_ref, c_ref, d_ref, cos_ref, sin_ref, mask_ref, first_ref, key_ref, value_ref, out_ref):
    packed = total_of([a_ref[...], b_ref[...], c_ref[...], d_ref[...]])
    batch = packed.shape[0]
    heads = packed.shape[1] // LANES - 3
    inverse = lax.rsqrt(packed[:, (heads + 2) * LANES :] / D + norm_eps)
    cosine, sine = cos_ref[...], sin_ref[...]

    def column(i):
        return packed[:, i * LANES : (i + 1) * LANES] * inverse

    def rotated(i):
        u = column(i)
        return (u * cosine + pltpu.roll(u, LANES // 2, 1) * sine).astype(jnp.bfloat16)

    queries = [rotated(h) for h in range(heads)]
    new_key = rotated(heads).astype(jnp.float32)
    new_value = column(heads + 1).astype(jnp.bfloat16).astype(jnp.float32)
    query = jnp.concatenate(queries, axis=0)
    keys = key_ref[layer, :, 0].reshape(batch * LANES, LANES)
    values = value_ref[layer, :, 0].reshape(batch * LANES, LANES)
    scores = lax.dot_general(
        query, keys, (((1,), (1,)), ((), ())), preferred_element_type=jnp.float32
    )
    row = lax.broadcasted_iota(jnp.int32, (batch, LANES), 0)
    usable = mask_ref[...] > 0.0
    first = first_ref[...] > 0.0
    tops, sums, fresh_all, weights = [], [], [], []
    for h in range(heads):
        block = scores[h * batch : (h + 1) * batch, :]
        mine = block[:, :LANES]
        for b in range(1, batch):
            mine = jnp.where(row == b, block[:, b * LANES : (b + 1) * LANES], mine)
        mine = jnp.where(usable, mine * scale, mask_fill)
        own = jnp.sum(queries[h].astype(jnp.float32) * new_key, axis=1, keepdims=True) * scale
        own = jnp.where(first, own, mask_fill)
        top = jnp.maximum(jnp.max(mine, axis=1, keepdims=True), own)
        weight = jnp.where(usable, jnp.exp(mine - top), 0.0)
        fresh = jnp.where(first, jnp.exp(own - top), 0.0)
        sums.append(jnp.sum(weight, axis=1, keepdims=True) + fresh)
        tops.append(jnp.broadcast_to(top, (batch, LANES)))
        fresh_all.append(fresh.astype(jnp.bfloat16).astype(jnp.float32))
        weights.append(
            jnp.concatenate(
                [jnp.where(row == b, weight, 0.0).astype(jnp.bfloat16) for b in range(batch)], axis=1
            )
        )
    context = jnp.dot(jnp.concatenate(weights, axis=0), values, preferred_element_type=jnp.float32)
    lane = lax.broadcasted_iota(jnp.int32, (batch, LANES), 1)
    stats = jnp.zeros((batch, LANES), jnp.float32)
    for h in range(heads):
        out_ref[:, h * LANES : (h + 1) * LANES] = (
            context[h * batch : (h + 1) * batch, :] + fresh_all[h] * new_value
        )
        stats = jnp.where(lane == h, tops[h], stats)
        stats = jnp.where(lane == heads + h, sums[h], stats)
    out_ref[:, heads * LANES :] = stats


def merged(refs):
    shards = [r[...] for r in refs]
    heads = shards[0].shape[1] // LANES - 1
    batch = shards[0].shape[0]
    stats = [s[:, heads * LANES :] for s in shards]
    lane = lax.broadcasted_iota(jnp.int32, (batch, LANES), 1)
    is_top = lane < heads
    tops = [jnp.where(is_top, s, 0.0) for s in stats]
    top = jnp.maximum(jnp.maximum(tops[0], tops[1]), jnp.maximum(tops[2], tops[3]))
    factors = [jnp.exp(t - top) for t in tops]
    total = jnp.zeros((batch, LANES), jnp.float32)
    for f, s in zip(factors, stats):
        total = total + pltpu.roll(f, heads, 1) * s
    outs = []
    for h in range(heads):
        cols = slice(h * LANES, (h + 1) * LANES)
        outs.append(total_of([f[:, h : h + 1] * s[:, cols] for f, s in zip(factors, shards)]))
    return outs, jnp.where(is_top, top, total), total


def merge_kernel(a_ref, b_ref, c_ref, d_ref, out_ref):
    outs, stats, _ = merged((a_ref, b_ref, c_ref, d_ref))
    heads = len(outs)
    for h in range(heads):
        out_ref[:, h * LANES : (h + 1) * LANES] = outs[h]
    out_ref[:, heads * LANES :] = stats


def output_kernel(layer, a_ref, b_ref, c_ref, d_ref, wo_ref, out_ref):
    outs, _, total = merged((a_ref, b_ref, c_ref, d_ref))
    heads = len(outs)
    context = jnp.concatenate(
        [(outs[h] / total[:, heads + h : heads + h + 1]).astype(jnp.bfloat16) for h in range(heads)],
        axis=1,
    )
    out_ref[...] = jnp.dot(context, wo_ref[layer], preferred_element_type=jnp.float32)


def on_device(hidden, norm_gains, w_query, w_key, w_value, w_out, key_cache, value_cache, lengths):
    batch = hidden.shape[0]
    width = key_cache.shape[4]
    location_total = key_cache.shape[3]
    heads = w_query.shape[2] // width
    scale = 1.0 / math.sqrt(width)
    ctx_index = lax.axis_index(CTX)
    positions = ctx_index * location_total + jnp.arange(location_total, dtype=jnp.int32)
    usable = (positions[None, :] < lengths[:, None]).astype(jnp.float32)
    first = jnp.broadcast_to(ctx_index == 0, (batch, 1)).astype(jnp.float32)
    exponents = jnp.arange(width // 2, dtype=jnp.float32) * (2.0 / width)
    frequency = jnp.exp(-exponents * math.log(rope_base))
    angles = lengths.astype(jnp.float32)[:, None] * frequency[None, :]
    cosine, sine = jnp.cos(angles), jnp.sin(angles)
    cosine = jnp.concatenate([cosine, cosine], axis=1)
    sine = jnp.concatenate([-sine, sine], axis=1)

    f32 = jnp.float32
    packed_shape = jax.ShapeDtypeStruct((batch, (heads + 3) * width), f32)
    stream_shape = jax.ShapeDtypeStruct(hidden.shape, f32)
    mixed_shape = jax.ShapeDtypeStruct((batch, (heads + 1) * width), f32)
    weights = (norm_gains, w_query, w_key, w_value)
    parts = None
    for layer in range(w_query.shape[0]):
        if layer == 0:
            packed, stream = first_project((packed_shape, stream_shape), hidden, *weights)
            w_out_first = fetch_first(w_out, packed)
        else:
            packed, stream = call(
                functools.partial(project_kernel, layer), (packed_shape, stream_shape), *parts, *weights
            )
        packed = sum_of(*exchange(packed, "x"))
        mixed = call(
            functools.partial(attend_kernel, layer, scale),
            mixed_shape,
            *exchange(packed, "y"), cosine, sine, usable, first, key_cache, value_cache,
        )
        mixed = call(merge_kernel, mixed_shape, *exchange(mixed, "x"))
        head_part = call(
            functools.partial(output_kernel, layer),
            stream_shape,
            *exchange(mixed, "y"),
            w_out if layer else w_out_first,
        )
        head_part = sum_of(head_part, lax.ppermute(head_part, "core", ((0, 1), (1, 0))))
        parts = [stream] + across(head_part)
    return sum_of(*parts)


def solution(mesh):
    finer = Mesh(mesh.devices.reshape(4, 4, 4, 2), ("y", "x", "z", "core"))
    tp = ("z", "core")
    return jax.shard_map(
        on_device,
        mesh=finer,
        in_specs=(
            P(None, CTX),
            P(None, CTX),
            P(None, CTX, tp),
            P(None, CTX, tp),
            P(None, CTX, tp),
            P(None, tp, CTX),
            P(None, None, tp, CTX, None),
            P(None, None, tp, CTX, None),
            P(),
        ),
        out_specs=P(None, CTX),
        check_vma=False,
    )
```
